256 devices in a mesh: rep: 1, dp: 256 (over x, y, z, core).
Axes of the slice: x: 4, y: 4, z: 8, core: 2. Of those that a mesh axis runs over, the one named last changes fastest.
Arguments:
- x: bfloat16 [256, 1024, 1024], P(('rep', 'dp'))
- dy: bfloat16 [256, 1024, 1024], P(('rep', 'dp'))
- w_gate: bfloat16 [2, 1024, 4096], P(None, 'dp')
- w_up: bfloat16 [2, 1024, 4096], P(None, 'dp')
- w_down: bfloat16 [2, 4096, 1024], P(None, 'dp')
Outputs:
- output 1: bfloat16 [256, 1024, 1024], P(('rep', 'dp'))
- output 2: bfloat16 [2, 1024, 4096], P('rep', 'dp')
- output 3: bfloat16 [2, 1024, 4096], P('rep', 'dp')
- output 4: bfloat16 [2, 4096, 1024], P('rep', 'dp')
All inputs are finite; a program needn't handle non-finite values.
Results may differ from the reference program's by a relative error of at most 0.018.
Values are sent between devices in bfloat16 or wider.
A program may use at most 768 MiB of HBM per device.

```python
import jax
import jax.numpy as jnp
from jax import lax

SEQUENCES = 256
TOKENS = 1024
D = 1024
FF = 4096
LAYERS = 2
NAMES = ("w_gate", "w_up", "w_down")
SHAPES = {"w_gate": (LAYERS, D, FF), "w_up": (LAYERS, D, FF), "w_down": (LAYERS, FF, D)}


def bump(key, n, height):
    away = (jnp.arange(n, dtype=jnp.int32) - jax.random.randint(key, (), 0, n, jnp.int32)) % n
    return jnp.where(away < n // 8, height, 1.0)


def together(key, own, strength):
    shared = jax.random.normal(key, own.shape[1:], jnp.float32)
    return (own + strength * shared) * lax.rsqrt(1 + strength * strength)


def setup_inputs(seed: int = 0, part: int = 0) -> dict:
    kx, kdy, ka, kb, kz, kf, kh, kl, *kw = jax.random.split(jax.random.key(seed), 8 + len(NAMES))
    kx, kdy, ka, kb = (jax.random.fold_in(k, part) for k in (kx, kdy, ka, kb))
    shape = (SEQUENCES, TOKENS, D)
    much_x, much_dy = jax.random.uniform(kz, (2,), jnp.float32, 0.0, 1.0)
    layers = 2.0 ** jax.random.uniform(kl, (LAYERS, 1, 1), jnp.float32, -1.0, 1.0)
    x = together(ka, jax.random.normal(kx, shape, jnp.float32), much_x) * bump(kf, D, 4.0)
    dy = together(kb, jax.random.normal(kdy, shape, jnp.float32), much_dy)
    drawn = {"x": x.astype(jnp.bfloat16), "dy": (dy * (SEQUENCES * TOKENS) ** -0.5).astype(jnp.bfloat16)}
    for key, name in zip(kw, NAMES, strict=True):
        w = jax.random.normal(key, SHAPES[name], jnp.float32) * SHAPES[name][1] ** -0.5
        drawn[name] = (w * {"w_gate": 1.0, "w_up": bump(kh, FF, 4.0), "w_down": layers}[name]).astype(jnp.bfloat16)
    return drawn


def matmul(a, w):
    return jnp.dot(a, w, preferred_element_type=jnp.float32).astype(jnp.bfloat16)


def normed(h):
    wide = h.astype(jnp.float32)
    scale = lax.rsqrt(jnp.mean(wide**2, -1, keepdims=True) + 1e-6)
    return (wide * scale).astype(jnp.bfloat16)


def layer(h, w):
    a = normed(h)
    gate = jnp.dot(a, w["w_gate"], preferred_element_type=jnp.float32)
    up = jnp.dot(a, w["w_up"], preferred_element_type=jnp.float32)
    return h + matmul((jax.nn.silu(gate) * up).astype(jnp.bfloat16), w["w_down"])


def stack(weights, h):
    return lax.scan(lambda h, w: (layer(h, w), None), h, weights)[0]


def reference(x, dy, w_gate, w_up, w_down):
    weights = dict(zip(NAMES, (w_gate, w_up, w_down), strict=True))

    def take(so_far, sequence):
        h, by_y = sequence
        _, back = jax.vjp(stack, weights, h)
        by_weights, by_h = back(by_y)
        return jax.tree.map(lambda total, term: total + term.astype(jnp.float32), so_far, by_weights), by_h

    none_yet = {name: jnp.zeros(w.shape, jnp.float32) for name, w in weights.items()}
    by_weights, by_x = lax.scan(take, none_yet, (x, dy))
    return (by_x, *(by_weights[name].astype(jnp.bfloat16) for name in NAMES))
```

```python
import functools
import heapq

import jax
import jax.numpy as jnp
from jax import lax
from jax.experimental import pallas as pl
from jax.experimental.pallas import tpu as pltpu
from jax.sharding import PartitionSpec as P

F32, BF16 = jnp.float32, jnp.bfloat16
MESH = pl.DeviceIdType.MESH
AXES = ("x", "y", "z")
DIMS = {256: (4, 4, 8), 128: (4, 4, 4), 64: (4, 4, 2), 32: (4, 2, 2), 16: (2, 2, 2)}
ORDERS = (("x", "y", "z"), ("z", "y", "x"), ("z", "x", "y"))
EPS = 1e-6
VMEM_LIMIT = 63 * 1024 * 1024


class Place:
    def __init__(self, dims):
        self.dims = dict(zip(AXES, dims, strict=True))
        nx, ny, nz = dims
        me = lax.axis_index("dp")
        self.core = me % 2
        self.other = 1 - self.core
        self.partner = me + 1 - 2 * self.core
        self.at = {"x": me // (2 * nz * ny), "y": (me // (2 * nz)) % ny, "z": (me // 2) % nz}

    def along(self, axis, by):
        n = self.dims[axis]
        return (self.at[axis] + (by % n)) % n

    def neighbour(self, axis, by):
        at = dict(self.at)
        at[axis] = self.along(axis, by)
        return ((at["x"] * self.dims["y"] + at["y"]) * self.dims["z"] + at["z"]) * 2 + self.core

    def barrier(self):
        semaphore = pltpu.get_barrier_semaphore()
        peers = [self.neighbour(axis, by) for axis in AXES for by in (1, -1)] + [self.partner]
        for peer in peers:
            pl.semaphore_signal(semaphore, inc=1, device_id={"dp": peer}, device_id_type=MESH)
        pl.semaphore_wait(semaphore, len(peers))


def piece(ref, index, tall, half=None, sub=None):
    rows, columns = ref.shape[-2:]
    length = rows if tall else columns
    start = 0
    if half is not None:
        length //= 2
        start = half * length
    if sub is not None:
        length //= 2
        start = start + sub * length
    if half is None and sub is None:
        cut = slice(None)
    else:
        cut = pl.ds(pl.multiple_of(start, 8 if tall else 128) if half is not None else start, length)
    return ref.at[(*index, cut, slice(None))] if tall else ref.at[(*index, slice(None), cut)]


def messages(dims, order):
    dims = dict(zip(AXES, dims, strict=True))
    return [(k, s, d) for k, axis in enumerate(order) for s in range(1, dims[axis] // 2 + 1) for d in (0, 1)]


class Gather:
    def __init__(self, place, dims, which, buffer, send, receive, pass_send, pass_receive):
        self.place, self.order, self.tall = place, ORDERS[which], which == 2
        self.buffer, self.send, self.receive = buffer, send, receive
        self.pass_send, self.pass_receive = pass_send.at[which], pass_receive.at[which]
        self.ids = {m: i for i, m in enumerate(messages(dims, self.order))}

    def half_length(self, k):
        return self.place.dims[self.order[k]] // 2

    def region(self, k, s, d, behind):
        axis = self.order[k]
        by = -behind if d == 0 else behind
        index = [
            slice(None) if a in self.order[:k] else self.place.along(a, by if a == axis else 0) for a in AXES
        ]
        return piece(self.buffer, index, self.tall, self.place.core, None if s < self.half_length(k) else d)

    def ring(self, k, s, d):
        region = self.region(k, s, d, s - 1)
        i = self.ids[k, s, d]
        peer = self.place.neighbour(self.order[k], 1 if d == 0 else -1)
        return pltpu.make_async_remote_copy(
            region, region, self.send.at[i], self.receive.at[i], device_id={"dp": peer}, device_id_type=MESH
        )

    def pass_on(self, region):
        return pltpu.make_async_remote_copy(
            region, region, self.pass_send, self.pass_receive, device_id={"dp": self.place.partner}, device_id_type=MESH
        )

    def begin(self):
        self.ring(0, 1, 0).start()
        self.ring(0, 1, 1).start()
        index = [self.place.at[a] for a in AXES]
        self.pass_on(piece(self.buffer, index, self.tall, self.place.core)).start()

    def take(self, k, s, d):
        self.ring(k, s, d).wait_recv()
        if s < self.half_length(k):
            self.ring(k, s + 1, d).start()
        elif d == 1 and k < 2:
            self.ring(k + 1, 1, 0).start()
            self.ring(k + 1, 1, 1).start()
        self.pass_on(self.region(k, s, d, s)).start()

    def finish(self):
        blocks = [slice(None)] * 3
        self.pass_on(piece(self.buffer, blocks, self.tall, self.place.other)).wait_recv()

    def drain(self):
        for m in self.ids:
            self.ring(*m).wait_send()
        blocks = [slice(None)] * 3
        self.pass_on(piece(self.buffer, blocks, self.tall, self.place.core)).wait_send()


LINK, LATENCY = 46.6e3, 2.2


def gather_plan(dims, block_bytes, start=(0.0, 0.0, 0.0), grid=None):
    sizes = dict(zip(AXES, dims, strict=True))
    free, heap, out = {}, [], []

    def post(t, m, k, s, d):
        axis = ORDERS[m][k]
        blocks = 1
        for a in ORDERS[m][:k]:
            blocks *= sizes[a]
        size = block_bytes / 2 * blocks * (0.5 if s == sizes[axis] // 2 else 1)
        begin = max(t, free.get((axis, d), 0.0))
        free[axis, d] = begin + size / LINK
        heapq.heappush(heap, (begin + size / LINK + LATENCY, m, k, s, d))

    for m, t in enumerate(start):
        post(t, m, 0, 1, 0)
        post(t, m, 0, 1, 1)
    got = {}
    while heap:
        t, m, k, s, d = heapq.heappop(heap)
        if grid is not None:
            t = grid * -(-t // grid)
        got.setdefault((m, k, s), []).append(d)
        h = sizes[ORDERS[m][k]] // 2
        if s < h:
            out.append((t, m, (k, s, d)))
            post(t, m, k, s + 1, d)
        elif len(got[m, k, s]) == 2:
            out.append((t, m, (k, s, 0)))
            out.append((t, m, (k, s, 1)))
            if k < 2:
                post(t, m, k + 1, 1, 0)
                post(t, m, k + 1, 1, 1)
    return out


def gather_scratch(dims, sizes):
    depth, width = sizes
    wide = (*dims, 8, width)
    counts = [len(messages(dims, order)) for order in ORDERS]
    return [
        pltpu.VMEM(wide, BF16),
        pltpu.VMEM(wide, BF16),
        pltpu.VMEM((*dims, 32, depth), BF16),
        pltpu.VMEM((2, 4, width // 2), BF16),
        pltpu.VMEM((2, 8, width // 2), F32),
        *[pltpu.SemaphoreType.DMA((n,)) for n in counts],
        *[pltpu.SemaphoreType.DMA((n,)) for n in counts],
        pltpu.SemaphoreType.DMA((3,)),
        pltpu.SemaphoreType.DMA((3,)),
        pltpu.SemaphoreType.DMA((2,)),
        pltpu.SemaphoreType.DMA((2,)),
        pltpu.SemaphoreType.DMA((4,)),
    ]


class LayerGather:
    def __init__(self, dims, shards, outs, scratch):
        self.place = Place(dims)
        self.shards, self.outs = shards, outs
        self.buffers = scratch[:3]
        self.peer_rows, self.wide_rows = scratch[3:5]
        sends, receives = scratch[5:8], scratch[8:11]
        pass_send, pass_receive, self.swap_send, self.swap_receive, self.local = scratch[11:16]
        self.matrices = [
            Gather(self.place, dims, m, self.buffers[m], sends[m], receives[m], pass_send, pass_receive) for m in range(3)
        ]

    def halves(self, ref, core):
        width = ref.shape[-1] // 2
        return ref.at[:, pl.ds(pl.multiple_of(core * width, 128), width)]

    def swap(self, m):
        return pltpu.make_async_remote_copy(
            self.halves(self.shards[m], self.place.other),
            self.peer_rows.at[m],
            self.swap_send.at[m],
            self.swap_receive.at[m],
            device_id={"dp": self.place.partner},
            device_id_type=MESH,
        )

    def begin(self):
        place = self.place
        at = [place.at[a] for a in AXES]
        self.swap(0).start()
        self.swap(1).start()
        down = pltpu.make_async_copy(
            self.shards[2], piece(self.buffers[2], at, True, place.core), self.local.at[3]
        )
        down.start()
        down.wait()
        self.matrices[2].begin()
        for m in range(2):
            self.swap(m).wait_recv()
            mine = self.shards[m][:, pl.ds(pl.multiple_of(place.core * (self.shards[m].shape[1] // 2), 128), self.shards[m].shape[1] // 2)]
            theirs = self.peer_rows[m]

            @pl.when(place.core == 0)
            def _():
                self.wide_rows[m, 0:4] = mine.astype(F32)
                self.wide_rows[m, 4:8] = theirs.astype(F32)

            @pl.when(place.core == 1)
            def _():
                self.wide_rows[m, 0:4] = theirs.astype(F32)
                self.wide_rows[m, 4:8] = mine.astype(F32)

            width = self.shards[m].shape[1] // 2
            self.buffers[m][(*at, slice(None), pl.ds(pl.multiple_of(place.core * width, 128), width))] = self.wide_rows[
                m
            ].astype(BF16)
        for m in range(2):
            self.matrices[m].begin()

    def take(self, m, message):
        self.matrices[m].take(*message)

    def store(self, m):
        return pltpu.make_async_copy(self.buffers[m], self.outs[m], self.local.at[m])

    def finish(self):
        for m in range(3):
            self.matrices[m].finish()
            self.store(m).start()
        for m in range(2):
            self.swap(m).wait_send()
        for m in range(3):
            self.matrices[m].drain()
        for m in range(3):
            self.store(m).wait()


def gather_kernel(dims, plan, gate, up, down, gate_out, up_out, down_out, *scratch):
    work = LayerGather(dims, (gate, up, down), (gate_out, up_out, down_out), scratch)
    work.place.barrier()
    work.begin()
    for _, m, message in plan:
        work.take(m, message)
    work.finish()


def weights_shapes(dims, depth, width):
    return [
        jax.ShapeDtypeStruct((*dims, 8, width), BF16),
        jax.ShapeDtypeStruct((*dims, 8, width), BF16),
        jax.ShapeDtypeStruct((*dims, 32, depth), BF16),
    ]


def gather(dims, gate, up, down, collective_id):
    width, depth = gate.shape[1], down.shape[1]
    outs = pl.pallas_call(
        functools.partial(gather_kernel, dims, gather_plan(dims, 16 * width)),
        out_shape=weights_shapes(dims, depth, width),
        in_specs=[pl.BlockSpec(memory_space=pltpu.VMEM)] * 2 + [pl.BlockSpec(memory_space=pl.ANY)],
        out_specs=[pl.BlockSpec(memory_space=pl.ANY)] * 3,
        scratch_shapes=gather_scratch(dims, (depth, width)),
        compiler_params=pltpu.CompilerParams(
            collective_id=collective_id, has_side_effects=True, vmem_limit_bytes=VMEM_LIMIT
        ),
        name=f"gather_{collective_id}",
    )(gate, up, down)
    return [out.reshape(-1, out.shape[-1]) for out in outs]


class Scatter:
    def __init__(self, place, dims, which, grad, own, theirs, short, full, send, receive, load, swap_send, swap_receive):
        self.place, self.order, self.tall = place, ORDERS[which][::-1], which == 2
        self.grad, self.own, self.theirs, self.short, self.full = grad, own, theirs, short, full
        self.send, self.receive = send, receive
        self.load_sem, self.swap_send, self.swap_receive = load, swap_send, swap_receive
        self.ids = {m: i for i, m in enumerate(messages(dims, self.order))}

    def half_length(self, k):
        return self.place.dims[self.order[k]] // 2

    def chunks(self):
        h = self.half_length(0)
        return [h, *[by for s in range(h - 1, 0, -1) for by in (s, -s)], 0]

    def chunk_index(self, by):
        return [self.place.along(a, by) if a == self.order[0] else slice(None) for a in AXES]

    def load(self, i):
        index = self.chunk_index(self.chunks()[i])
        return pltpu.make_async_copy(
            piece(self.grad, index, self.tall, self.place.core), self.own.at[tuple(index)], self.load_sem.at[i]
        )

    def swap(self, i):
        index = self.chunk_index(self.chunks()[i])
        return pltpu.make_async_remote_copy(
            piece(self.grad, index, self.tall, self.place.other),
            self.theirs.at[tuple(index)],
            self.swap_send.at[i],
            self.swap_receive.at[i],
            device_id={"dp": self.place.partner},
            device_id_type=MESH,
        )

    def begin(self, i):
        self.swap(i).start()
        self.load(i).start()

    def ready(self, i):
        self.load(i).wait()
        self.swap(i).wait_recv()

    def index(self, k, by):
        return [
            slice(None) if a in self.order[k + 1 :] else self.place.along(a, by if self.order[k : k + 1] == (a,) else 0)
            for a in AXES
        ]

    def ring(self, k, s, d):
        h = self.half_length(k)
        by = h - s + 1 if d == 0 else -(h - s + 1)
        source = piece(self.own, self.index(k, by), self.tall, sub=d if s == 1 else None)
        landing = self.short[k].at[d] if s == 1 else self.full[k].at[d, s - 2]
        i = self.ids[k, s, d]
        peer = self.place.neighbour(self.order[k], 1 if d == 0 else -1)
        return pltpu.make_async_remote_copy(
            source, landing, self.send.at[i], self.receive.at[i], device_id={"dp": peer}, device_id_type=MESH
        )

    def terms(self, k, index):
        whole, quarters = [self.own.at[tuple(index)], self.theirs.at[tuple(index)]], ([], [])
        for j in range(k):
            at = [index[AXES.index(a)] for a in AXES if a in self.order[j + 1 :]]
            h = self.half_length(j)
            for d in (0, 1):
                if h == 1:
                    quarters[d].append(self.short[j].at[(d, *at)])
                else:
                    whole.append(self.full[j].at[(d, h - 2, *at)])
        return whole, quarters

    def add(self, k, by, arrived=None, out=None):
        free = [a for a in AXES if a in self.order[k + 1 :]]
        sizes = [self.place.dims[a] for a in free]
        count = 1
        for n in sizes:
            count *= n
        fixed = self.index(k, by)

        def one(i):
            at, rest = {}, i
            for a, n in reversed(list(zip(free, sizes, strict=True))):
                at[a], rest = (rest % n, rest // n) if a != free[0] else (rest, 0)
            index = [at[a] if a in free else fixed[j] for j, a in enumerate(AXES)]
            whole, quarters = self.terms(k, index)
            whole, quarters = list(whole), (list(quarters[0]), list(quarters[1]))
            place = [at[a] for a in free]
            if arrived is not None:
                s, d = arrived
                if s == 1:
                    quarters[d].append(self.short[k].at[(d, *place)])
                else:
                    whole.append(self.full[k].at[(d, s - 2, *place)])
            target = self.own.at[tuple(index)] if out is None else out
            for q in (0, 1):
                length = target.shape[0 if self.tall else 1] // 2
                cut = (slice(q * length, (q + 1) * length), slice(None))
                cut = cut if self.tall else cut[::-1]
                total = None
                for ref in whole:
                    value = ref[cut].astype(F32)
                    total = value if total is None else total + value
                for ref in quarters[q]:
                    total = total + ref[...].astype(F32)
                target[cut] = total.astype(BF16)

        if count == 1:
            one(0)
        else:
            pl.loop(0, count)(one)

    def first(self, k):
        h = self.half_length(k)
        if k == 0:
            self.ready(0)
        self.add(k, h)
        self.ring(k, 1, 0).start()
        self.ring(k, 1, 1).start()

    def take(self, k, s, d):
        h = self.half_length(k)
        self.ring(k, s, d).wait_recv()
        if s < h:
            by = h - s if d == 0 else -(h - s)
            if k == 0:
                self.ready(self.chunks().index(by))
            self.add(k, by, (s, d))
            self.ring(k, s + 1, d).start()
        elif d == 1:
            if k == 0:
                self.ready(len(self.chunks()) - 1)
            if k < 2:
                self.first(k + 1)

    def result(self, out):
        self.add(3, 0, out=out)

    def drain(self):
        for m in self.ids:
            self.ring(*m).wait_send()
        for i in range(len(self.chunks())):
            self.swap(i).wait_send()


D2D, HBM, ADD = 500e3, 3000e3, 250e3


def scatter_plan(dims, block_bytes, grid=None):
    sizes = dict(zip(AXES, dims, strict=True))
    chips = dims[0] * dims[1] * dims[2]
    orders = [order[::-1] for order in ORDERS]
    free, heap, out = {}, [], []
    swapped, swap_time = {}, LATENCY + 1.0
    hs = [[sizes[a] // 2 for a in order] for order in orders]
    lists = [[h[0], *[by for s in range(h[0] - 1, 0, -1) for by in (s, -s)], 0] for h in hs]
    queue = sorted(((i + 1) / len(c), m, by) for m, c in enumerate(lists) for i, by in enumerate(c))
    for _, m, by in queue:
        swap_time += block_bytes / 2 * chips / sizes[orders[m][0]] / D2D
        swapped[m, by] = swap_time

    def size_of(m, k):
        blocks = 1
        for a in orders[m][k + 1 :]:
            blocks *= sizes[a]
        return block_bytes / 2 * blocks

    def post(t, m, k, s, d):
        size = size_of(m, k) * (0.5 if s == 1 else 1)
        begin = max(t, free.get((orders[m][k], d), 0.0))
        free[orders[m][k], d] = begin + size / LINK
        ready = begin + size / LINK + LATENCY
        h = hs[m][k]
        if k == 0 and s <= h:
            by = (h - s) * (1 if d == 0 else -1)
            ready = max(ready, swapped[m, by if s < h else 0])
        heapq.heappush(heap, (ready, m, k, s, d))

    clock = 0.0
    for m in range(3):
        heapq.heappush(heap, (swapped[m, hs[m][0]], m, -1, 0, 0))
    got = {}
    while heap:
        ready, m, k, s, d = heapq.heappop(heap)
        t = max(ready, clock)
        if grid is not None:
            t = max(clock, grid * -(-ready // grid))
        if k < 0:
            clock = t + size_of(m, 0) / ADD
            out.append((t, m, None))
            post(clock, m, 0, 1, 0)
            post(clock, m, 0, 1, 1)
            continue
        h = hs[m][k]
        if s < h:
            clock = t + size_of(m, k) / ADD
            out.append((t, m, (k, s, d)))
            post(clock, m, k, s + 1, d)
            continue
        got.setdefault((m, k), []).append(d)
        if len(got[m, k]) == 2:
            out.append((t, m, (k, s, 0)))
            out.append((t, m, (k, s, 1)))
            if k < 2:
                clock = t + size_of(m, k + 1) / ADD
                post(clock, m, k + 1, 1, 0)
                post(clock, m, k + 1, 1, 1)
    return out, [(m, lists[m].index(by)) for _, m, by in queue]


def scatter_scratch(dims, depth, width):
    sizes = dict(zip(AXES, dims, strict=True))
    out = []
    for m, order in enumerate(ORDERS):
        order = order[::-1]
        block = (16, depth) if m == 2 else (8, width // 2)
        short = (8, depth) if m == 2 else (8, width // 4)
        out += [pltpu.VMEM((*dims, *block), BF16)] * 2
        for k, axis in enumerate(order):
            rest = [sizes[a] for a in AXES if a in order[k + 1 :]]
            h = sizes[axis] // 2
            out.append(pltpu.VMEM((2, *rest, *short), BF16))
            if h > 1:
                out.append(pltpu.VMEM((2, h - 1, *rest, *block), BF16))
        n, c = len(messages(dims, order)), sizes[order[0]]
        out += [pltpu.SemaphoreType.DMA((n,))] * 2 + [pltpu.SemaphoreType.DMA((c,))] * 3
    out += [pltpu.VMEM((2, 8, width // 2), BF16), pltpu.VMEM((2, 8, width // 2), BF16)]
    out += [pltpu.SemaphoreType.DMA((2,))] * 2 + [pltpu.SemaphoreType.DMA((1,)), pltpu.VMEM((16, depth), BF16)]
    return out


class LayerScatter:
    def __init__(self, dims, grads, outs, scratch):
        self.place, self.outs = Place(dims), outs
        scratch = list(scratch)
        self.matrices = []
        for m in range(3):
            own, theirs = scratch.pop(0), scratch.pop(0)
            short, full = [], []
            for axis in ORDERS[m][::-1]:
                short.append(scratch.pop(0))
                full.append(scratch.pop(0) if self.place.dims[axis] > 2 else None)
            semaphores = [scratch.pop(0) for _ in range(5)]
            self.matrices.append(Scatter(self.place, dims, m, grads[m], own, theirs, short, full, *semaphores))
        self.mine, self.peer, self.send, self.receive, self.local, self.down = scratch

    def begin(self, loads):
        for m, i in loads:
            self.matrices[m].begin(i)

    def take(self, m, message):
        if message is None:
            self.matrices[m].first(0)
        else:
            self.matrices[m].take(*message)

    def swap(self, m):
        return pltpu.make_async_remote_copy(
            self.mine.at[m],
            self.peer.at[m],
            self.send.at[m],
            self.receive.at[m],
            device_id={"dp": self.place.partner},
            device_id_type=MESH,
        )

    def finish(self):
        for m in range(2):
            self.matrices[m].result(self.mine.at[m])
        self.matrices[2].result(self.outs[2])
        for m in range(2):
            self.swap(m).start()
        for m in range(3):
            self.matrices[m].drain()
        for m in range(2):
            self.swap(m).wait_recv()
            mine, peer = self.mine[m].astype(F32), self.peer[m].astype(F32)
            width = mine.shape[1]

            @pl.when(self.place.core == 0)
            def _():
                self.outs[m][:, :width] = mine[0:4].astype(BF16)
                self.outs[m][:, width:] = peer[0:4].astype(BF16)

            @pl.when(self.place.core == 1)
            def _():
                self.outs[m][:, :width] = peer[4:8].astype(BF16)
                self.outs[m][:, width:] = mine[4:8].astype(BF16)

        for m in range(2):
            self.swap(m).wait_send()


def scatter_kernel(dims, plan, loads, gate, up, down, gate_out, up_out, down_out, *scratch):
    work = LayerScatter(dims, (gate, up, down), (gate_out, up_out, down_out), scratch)
    work.place.barrier()
    work.begin(loads)
    for _, m, message in plan:
        work.take(m, message)
    work.finish()


def scatter(dims, grads, collective_id):
    width, depth = grads[0].shape[1], grads[2].shape[1]
    shapes = weights_shapes(dims, depth, width)
    plan, loads = scatter_plan(dims, 16 * width)
    return pl.pallas_call(
        functools.partial(scatter_kernel, dims, plan, loads),
        out_shape=[
            jax.ShapeDtypeStruct((4, width), BF16),
            jax.ShapeDtypeStruct((4, width), BF16),
            jax.ShapeDtypeStruct((16, depth), BF16),
        ],
        in_specs=[pl.BlockSpec(memory_space=pl.ANY)] * 3,
        out_specs=[pl.BlockSpec(memory_space=pltpu.VMEM)] * 3,
        scratch_shapes=scatter_scratch(dims, depth, width),
        compiler_params=pltpu.CompilerParams(
            collective_id=collective_id, has_side_effects=True, vmem_limit_bytes=VMEM_LIMIT
        ),
        name=f"scatter_{collective_id}",
    )(*[g.reshape(s.shape) for g, s in zip(grads, shapes, strict=True)])


def dot(a, b, ca, cb):
    return lax.dot_general(a, b, (((ca,), (cb,)), ((), ())), preferred_element_type=F32)


def normed(h):
    wide = h.astype(F32)
    return (wide * lax.rsqrt(jnp.mean(wide * wide, -1, keepdims=True) + EPS)).astype(BF16)


def forward_kernel(h, gate, up, down, a_out, h_out, next_out, total):
    j, last = pl.program_id(0), pl.num_programs(0) - 1

    @pl.when(j == 0)
    def _():
        a_out[...] = normed(h[...])
        total[...] = jnp.zeros_like(total)

    a = a_out[...]
    g = dot(a, gate[...], 1, 0)
    u = dot(a, up[...], 1, 0)
    p = (g * jax.nn.sigmoid(g) * u).astype(BF16)
    total[...] += dot(p, down[...], 1, 0)

    @pl.when(j == last)
    def _():
        out = (h[...].astype(F32) + total[...].astype(BF16).astype(F32)).astype(BF16)
        h_out[...] = out
        next_out[...] = normed(out)


def forward(h, gate, up, down, tile=512):
    tokens, depth = h.shape
    tile = min(tile, gate.shape[1])
    whole = pl.BlockSpec((tokens, depth), lambda j: (0, 0))
    wide = pl.BlockSpec((depth, tile), lambda j: (0, j))
    tall = pl.BlockSpec((tile, depth), lambda j: (j, 0))
    return pl.pallas_call(
        forward_kernel,
        grid=(gate.shape[1] // tile,),
        out_shape=[jax.ShapeDtypeStruct((tokens, depth), BF16)] * 3,
        in_specs=[whole, wide, wide, tall],
        out_specs=[whole] * 3,
        scratch_shapes=[pltpu.VMEM((tokens, depth), F32)],
        compiler_params=pltpu.CompilerParams(vmem_limit_bytes=VMEM_LIMIT),
        cost_estimate=pl.CostEstimate(
            flops=6 * tokens * depth * gate.shape[1], bytes_accessed=6 * gate.size + 8 * h.size, transcendentals=0
        ),
        name="forward",
    )(h, gate, up, down)


def backward_kernel(a, h, dh, gate, up, down, dgate_out, dup_out, ddown_out, dh_out, total):
    j, last = pl.program_id(0), pl.num_programs(0) - 1

    @pl.when(j == 0)
    def _():
        total[...] = jnp.zeros_like(total)

    a_, dh_ = a[...], dh[...]
    gate_, up_ = gate[...], up[...]
    g = dot(a_, gate_, 1, 0)
    u = dot(a_, up_, 1, 0)
    s = jax.nn.sigmoid(g)
    silu = g * s
    ddown_out[...] = dot((silu * u).astype(BF16), dh_, 0, 0).astype(BF16)
    dp = dot(dh_, down[...], 1, 1).astype(BF16).astype(F32)
    du = (dp * silu).astype(BF16)
    dg = (dp * u * (s + silu * (1 - s))).astype(BF16)
    dgate_out[...] = dot(a_, dg, 0, 0).astype(BF16)
    dup_out[...] = dot(a_, du, 0, 0).astype(BF16)
    total[...] += dot(dg, gate_, 1, 1) + dot(du, up_, 1, 1)

    @pl.when(j == last)
    def _():
        wide = h[...].astype(F32)
        scale = lax.rsqrt(jnp.mean(wide * wide, -1, keepdims=True) + EPS)
        da = total[...].astype(BF16).astype(F32)
        along = jnp.mean(da * wide, -1, keepdims=True)
        dwide = scale * (da - wide * (scale * scale * along))
        dh_out[...] = (dh[...].astype(F32) + dwide.astype(BF16).astype(F32)).astype(BF16)


def backward(a, h, dh, gate, up, down, tile=512):
    tokens, depth = h.shape
    tile = min(tile, gate.shape[1])
    whole = pl.BlockSpec((tokens, depth), lambda j: (0, 0))
    wide = pl.BlockSpec((depth, tile), lambda j: (0, j))
    tall = pl.BlockSpec((tile, depth), lambda j: (j, 0))
    return pl.pallas_call(
        backward_kernel,
        grid=(gate.shape[1] // tile,),
        out_shape=[
            jax.ShapeDtypeStruct(gate.shape, BF16),
            jax.ShapeDtypeStruct(gate.shape, BF16),
            jax.ShapeDtypeStruct(down.shape, BF16),
            jax.ShapeDtypeStruct((tokens, depth), BF16),
        ],
        in_specs=[whole, whole, whole, wide, wide, tall],
        out_specs=[wide, wide, tall, whole],
        scratch_shapes=[pltpu.VMEM((tokens, depth), F32)],
        compiler_params=pltpu.CompilerParams(vmem_limit_bytes=VMEM_LIMIT),
        cost_estimate=pl.CostEstimate(
            flops=16 * tokens * depth * gate.shape[1], bytes_accessed=12 * gate.size + 8 * h.size, transcendentals=0
        ),
        name="backward",
    )(a, h, dh, gate, up, down)


def solution(mesh):
    dims = DIMS[mesh.shape["dp"]]

    def local(x, dy, w_gate, w_up, w_down):
        h, dh = x[0], dy[0]
        first = gather(dims, w_gate[0], w_up[0], w_down[0], 1)
        second = gather(dims, w_gate[1], w_up[1], w_down[1], 2)
        a1, h1, a2 = forward(h, *first)
        *grads2, dh1 = backward(a2, h1, dh, *second)
        sums2 = scatter(dims, grads2, 3)
        *grads1, dh0 = backward(a1, h, dh1, *first)
        sums1 = scatter(dims, grads1, 4)
        return (dh0[None], *(jnp.stack(both) for both in zip(sums1, sums2, strict=True)))

    rows = P(None, "dp", None)
    return jax.shard_map(
        local,
        mesh=mesh,
        in_specs=(P(("rep", "dp"), None, None),) * 2 + (rows,) * 3,
        out_specs=(P(("rep", "dp"), None, None),) + (P("rep", "dp", None),) * 3,
        check_vma=False,
    )
```

```python
import functools
import heapq

import jax
import jax.numpy as jnp
from jax import lax
from jax.experimental import pallas as pl
from jax.experimental.pallas import tpu as pltpu
from jax.sharding import PartitionSpec as P

F32, BF16 = jnp.float32, jnp.bfloat16
MESH = pl.DeviceIdType.MESH
ALL, BOTH, ANY = slice(None), (0, 1), pl.BlockSpec(memory_space=pl.ANY)
AXES = ("x", "y", "z")
DIMS = {256: (4, 4, 8)}
ORDERS = (("x", "y", "z"), ("z", "y", "x"), ("z", "x", "y"))
MATRICES = range(len(ORDERS))
ROWS = 8
EPS = 1e-6
PARAMS = functools.partial(pltpu.CompilerParams, vmem_limit_bytes=66_500_000, has_side_effects=True)

LINK, D2D, ADD, HOP, FURTHER, ACT = 46.6e3, 550e3, 2000e3, 2.3, 0.7, 0.05


class Place:
    def __init__(self, dims):
        self.dims = dict(zip(AXES, dims, strict=True))
        _, ny, nz = dims
        me = lax.axis_index("dp")
        chip = me // 2
        self.core = me % 2
        self.other = 1 - self.core
        self.partner = me + 1 - 2 * self.core
        self.at = {"x": chip // (nz * ny), "y": (chip // nz) % ny, "z": chip % nz}
        self.block = [self.at[a] for a in AXES]

    def along(self, axis, by):
        n = self.dims[axis]
        return (self.at[axis] + by % n) % n

    def neighbour(self, axis, by):
        at = {**self.at, axis: self.along(axis, by)}
        return ((at["x"] * self.dims["y"] + at["y"]) * self.dims["z"] + at["z"]) * 2 + self.core

    def everyone(self):
        return [self.neighbour(a, by) for a in AXES for by in range(1, self.dims[a])] + [self.partner]

    def tell(self, semaphore):
        for peer in self.everyone():
            pl.semaphore_signal(semaphore, inc=1, device_id={"dp": peer}, device_id_type=MESH)

    def hear(self, semaphore):
        pl.semaphore_wait(semaphore, len(self.everyone()))

    def barrier(self):
        self.tell(pltpu.get_barrier_semaphore())
        self.hear(pltpu.get_barrier_semaphore())

    def copy(self, source, target, send, receive, peer):
        return pltpu.make_async_remote_copy(source, target, send, receive, device_id={"dp": peer}, device_id_type=MESH)


def sub(ref, d):
    width = ref.shape[-1] // 2
    return ref.at[(*[ALL] * (len(ref.shape) - 1), pl.ds(d * width, width))]


def offsets(n):
    return [n // 2, *[by for s in range(n // 2 - 1, 0, -1) for by in (s, -s)], 0]


def lengths(dims, order):
    sizes = dict(zip(AXES, dims, strict=True))
    return [sizes[a] for a in order]


def ring_steps(n):
    return [(s, d) for s in range(1, n // 2 + 1) for d in BOTH]


def gather_messages(dims, order, flows):
    a, b, c = lengths(dims, order)
    return (
        [(0, by) for by in range(1, a)]
        + [(1, 0, *m) for m in ring_steps(b)]
        + [(2, g, *m) for g in gather_flows(b, flows) for m in ring_steps(c)]
    )


def gather_flows(n, flows):
    return offsets(n)[::-1] if flows else [None]


def scatter_messages(dims, order):
    a, b, c = lengths(dims, order)
    return (
        [(0, g, *m) for g in offsets(b) for m in ring_steps(a)]
        + [(1, 0, *m) for m in ring_steps(b)]
        + [(2, by) for by in range(1, c)]
    )


def simulate(actions, arrivals, stages, urgency, lead=4.0):
    times, waiting, users, heap, free = dict(arrivals), {}, {}, [], {}

    def put(at, name):
        at = max([at, *[free.get(link, 0.0) - lead for _, link, *_ in actions[name][1]]])
        heapq.heappush(heap, (at, urgency(name), len(times), str(name), name))

    def ready(name):
        put(max([times[n] for n in actions[name][0]], default=0.0), name)

    for name, (needs, *_) in actions.items():
        missing = [n for n in needs if n not in times]
        waiting[name] = len(missing)
        for n in missing:
            users.setdefault(n, []).append(name)
        if not missing:
            ready(name)
    clock, plan, done, seen = 0.0, [[]], set(), set()

    def do():
        nonlocal clock
        at, *_, name = heapq.heappop(heap)
        needs, sends, cost = actions[name]
        if any(free.get(link, 0.0) - lead > max(at, clock) for _, link, *_ in sends):
            put(at, name)
            return None
        clock = max(clock, at) + cost
        plan[-1].append((name, [n for n in needs if n not in seen]))
        seen.update(needs)
        done.add(name)
        for arrival, link, size, hops in sends:
            free[link] = max(clock, free.get(link, 0.0)) + hops * size / LINK
            times[arrival] = free[link] + HOP + FURTHER * (hops - 1)
            for user in users.get(arrival, ()):
                waiting[user] -= 1
                if not waiting[user]:
                    ready(user)
        return name

    for time, before in stages:
        left = set(before) - done
        while heap and (left or heap[0][0] <= clock):
            left.discard(do())
        plan.append([])
        clock += time
    while heap:
        do()
    return clock, plan


def gather_actions(dims, piece, unit, flows):
    actions = {}
    for m, order in enumerate(ORDERS):
        a, b, c = lengths(dims, order)
        half = [0, b // 2, c // 2]
        straight = [((unit, m, 0, by), (order[0], by * 2 > a), piece, min(by, a - by)) for by in range(1, a)]
        actions["begin", unit, m] = ([("begin", unit)], straight, 6 * ACT)
        first = [s[0] for s in straight]
        for k, g in [(1, 0)] + [(2, g) for g in gather_flows(b, flows)]:
            size = piece * a * (b if g is None else 1)
            if g and g < half[1]:
                needs = [(unit, m, 1, 0, abs(g), 0 if g < 0 else 1)]
            else:
                needs = first if g == 0 else [(unit, m, 1, 0, half[1], d) for d in BOTH]
            for s, d in [(1, None)] + [r for r in ring_steps(2 * half[k]) if r[0] > 1]:
                sends = [
                    ((unit, m, k, g, s, w), (order[k], w), size / (2 if s == half[k] else 1), 1)
                    for w in (BOTH if d is None else (d,))
                ]
                actions["send", unit, m, k, g, s, d] = (needs if s == 1 else [(unit, m, k, g, s - 1, d)], sends, ACT)
            if k == 2:
                actions["take", unit, m, g] = ([(unit, m, k, g, half[k], d) for d in BOTH], [], ACT)
    return actions


def gather_urgency(name):
    what, unit, _, *rest = name
    return (unit, rest[0], rest[2]) if what == "send" else (unit, 0, 0)


def scatter_urgency(name):
    what, unit, _, *rest = name
    return (unit, -rest[0], -abs(rest[1]), rest[2]) if what == "send" else (unit, -3, 0, 0)


def scatter_actions(dims, piece, unit=0, begin=2.0):
    actions, arrivals, queue = {}, {}, []
    for m, order in enumerate(ORDERS):
        order = order[::-1]
        a, b, c = lengths(dims, order)
        half = [a // 2, b // 2]
        size = [piece * c, piece * c]
        queue += [((i + 1) / a, m, i, by, piece * b * c) for i, by in enumerate(offsets(a))]

        def over(k, g):
            return [(unit, m, k, g, half[k], d) for d in BOTH]

        for k, g in [(0, g) for g in offsets(b)] + [(1, 0)]:
            for s, d in [(1, None)] + [r for r in ring_steps(2 * half[k]) if r[0] > 1]:
                by = (half[k] - s + 1) * (-1 if d else 1)
                needs = [(unit, m, "chunk", 0 if k else by)]
                if s > 1:
                    needs.append((unit, m, k, g, s - 1, d))
                if k:
                    needs += over(0, by)
                sends = [
                    ((unit, m, k, g, s, w), (order[k], w), size[k] / (2 if s == 1 else 1), 1)
                    for w in (BOTH if d is None else (d,))
                ]
                actions["send", unit, m, k, g, s, d] = (needs, sends, size[k] / ADD + ACT)
        straight = [((unit, m, 2, by), (order[2], by * 2 > c), piece, min(by, c - by)) for by in range(1, c)]
        actions["last", unit, m] = (over(0, 0) + over(1, 0), straight, 6 * ACT)
        actions["result", unit, m] = ([s[0] for s in straight], [], 4 * ACT)
    time, loads = begin + HOP, []
    for _, m, i, by, size in sorted(queue):
        time += size / D2D
        arrivals[unit, m, "chunk", by] = time
        loads.append((m, i))
    return actions, arrivals, loads


class Gather:
    def __init__(self, place, which, flows, buffer, sends, receives, pass_send, pass_receive):
        self.place, self.order, self.buffer, self.sends, self.receives = place, ORDERS[which], buffer, sends, receives
        self.passing = pass_send.at[which], pass_receive.at[which]
        self.n = [place.dims[a] for a in self.order]
        self.ids = {m: i for i, m in enumerate(gather_messages(place.dims.values(), self.order, flows))}

    def half(self, k, g, by=0):
        first, second, third = self.order
        if k == 0:
            where = {}
        elif k == 1:
            where = {first: ALL, second: by}
        else:
            where = {first: ALL, second: ALL if g is None else g, third: by}
        at = [where.get(a, 0) for a in AXES]
        index = [i if i is ALL else self.place.along(a, i) for a, i in zip(AXES, at, strict=True)]
        return self.buffer.at[(*index, self.place.core)]

    def copy(self, k, *rest):
        if k == 0:
            (to,) = rest
            region = self.half(k, 0)
        else:
            g, s, d = rest
            to = -1 if d else 1
            region = self.half(k, g, -to * (s - 1))
            if s == self.n[k] // 2:
                region = sub(region, d)
        i = self.ids[(k, *rest)]
        return self.place.copy(
            region, region, self.sends.at[i], self.receives.at[i], self.place.neighbour(self.order[k], to)
        )

    def begin(self):
        for by in range(1, self.n[0]):
            self.copy(0, by).start()

    def wait(self, *message):
        self.copy(*message).wait_recv()

    def send(self, k, g, s, d):
        for w in BOTH if d is None else (d,):
            self.copy(k, g, s, w).start()

    def pass_on(self, region):
        return self.place.copy(region, region, *self.passing, self.place.partner)

    def take(self, g):
        self.pass_on(self.half(2, g, ALL)).start()

    def passed(self, core):
        return self.pass_on(self.buffer.at[ALL, ALL, ALL, core])

    def finish(self):
        self.passed(self.place.other).wait_recv()

    def drain(self):
        for m in self.ids:
            self.copy(*m).wait_send()
        self.passed(self.place.core).wait_send()


def weights_shapes(dims, depth, rows=ROWS):
    return [jax.ShapeDtypeStruct((*dims, 2, rows, depth), BF16) for _ in MATRICES]


def gather_scratch(dims, depth, flows):
    three = pltpu.SemaphoreType.DMA((len(MATRICES),))
    return [
        *[pltpu.VMEM((*dims, 2, ROWS, depth), BF16) for _ in MATRICES],
        *[pltpu.VMEM((rows, depth), BF16) for rows in (ROWS // 2, ROWS // 2, ROWS)],
        *[pltpu.SemaphoreType.DMA((len(gather_messages(dims, o, flows)),)) for o in ORDERS * 2],
        *[three] * 5,
        pltpu.VMEM((2, ROWS, depth), F32),
    ]


class UnitGather:
    def __init__(self, place, half, flows, shards, outs, scratch):
        self.place, self.half, self.shards, self.outs = place, half, shards, outs
        scratch = iter(scratch)
        self.buffers = [next(scratch) for _ in MATRICES]
        self.peers = [next(scratch) for _ in MATRICES]
        sends, receives = [next(scratch) for _ in MATRICES], [next(scratch) for _ in MATRICES]
        pass_send, pass_receive, self.swap_send, self.swap_receive, self.local, self.rows = scratch
        self.matrices = [
            Gather(place, m, flows, self.buffers[m], sends[m], receives[m], pass_send, pass_receive) for m in MATRICES
        ]

    def swap(self, m):
        place = self.place
        return place.copy(
            self.shards[m].at[place.other], self.peers[m], self.swap_send.at[m], self.swap_receive.at[m], place.partner
        )

    def prepare(self, loads=()):
        for m in MATRICES:
            self.swap(m).start()

    def begin(self, m):
        self.swap(m).wait_recv()
        mine, peer = self.shards[m][self.place.core].astype(F32), self.peers[m][:].astype(F32)
        first = self.place.core == 0
        if m == len(MATRICES) - 1:
            block = jnp.where(self.place.core == self.half, mine, peer)
        else:
            self.rows[m, : ROWS // 2] = jnp.where(first, mine, peer)
            self.rows[m, ROWS // 2 :] = jnp.where(first, peer, mine)
            block = self.rows[m]
        self.buffers[m][(*self.place.block, self.place.core)] = block.astype(BF16)
        self.matrices[m].begin()

    def do(self, action, needs):
        what, _, m, *message = action
        matrix = self.matrices[m]
        if what == "begin":
            self.begin(m)
            return
        for _, _, *need in needs:
            matrix.wait(*need)
        if what == "send":
            matrix.send(*message)
        else:
            matrix.take(*message)

    def store(self, m):
        return pltpu.make_async_copy(self.buffers[m], self.outs[m], self.local.at[m])

    def finish(self):
        for m in MATRICES:
            self.matrices[m].finish()
            self.store(m).start()

    def drain(self):
        for m in MATRICES:
            self.swap(m).wait_send()
            self.matrices[m].drain()
            self.store(m).wait()


class Scatter:
    def __init__(self, place, which, grad, scratch):
        self.place, self.order, self.grad = place, ORDERS[which][::-1], grad
        self.n = [place.dims[a] for a in self.order]
        self.own, self.theirs = next(scratch), next(scratch)
        self.short, self.full = [], []
        for n in self.n[:2]:
            self.short.append(next(scratch))
            self.full.append(next(scratch) if n > 2 else None)
        self.straight, self.sends, self.receives, self.load_sem, *self.swap_sems = [next(scratch) for _ in range(6)]
        self.ids = {m: i for i, m in enumerate(scatter_messages(place.dims.values(), self.order))}
        self.chunks = offsets(self.n[0])

    def chunk(self, i):
        return [self.place.along(a, self.chunks[i]) if a == self.order[0] else ALL for a in AXES]

    def load(self, i):
        index = self.chunk(i)
        return pltpu.make_async_copy(
            self.grad.at[(*index, self.place.core)], self.own.at[tuple(index)], self.load_sem.at[i]
        )

    def swap(self, i):
        index, (send, receive) = self.chunk(i), self.swap_sems
        source = self.grad.at[(*index, self.place.other)]
        return self.place.copy(source, self.theirs.at[tuple(index)], send.at[i], receive.at[i], self.place.partner)

    def begin(self, i):
        self.swap(i).start()
        self.load(i).start()

    def wait(self, what, *rest):
        if what == "chunk":
            i = self.chunks.index(*rest)
            self.load(i).wait()
            self.swap(i).wait_recv()
        else:
            self.copy(what, *rest).wait_recv()

    def index(self, k, g, by):
        where = dict(zip(self.order[k : k + 2], (by, g), strict=False))
        free = self.order[max(k + 1, 2) :]
        return [ALL if a in free else self.place.along(a, where.get(a, 0)) for a in AXES]

    def landing(self, buffer, k, lead, index):
        return buffer.at[(*lead, *[i for a, i in zip(AXES, index, strict=True) if a in self.order[k + 1 :]])]

    def copy(self, k, *rest):
        if k == 2:
            (by,) = rest
            to, index = by, self.index(k, 0, by)
            source, landing = self.own.at[tuple(index)], self.straight.at[by - 1]
        else:
            g, s, d = rest
            to = -1 if d else 1
            index = self.index(k, g, to * (self.n[k] // 2 - s + 1))
            source = self.own.at[tuple(index)]
            if s == 1:
                source, landing = sub(source, d), self.landing(self.short[k], k, (d,), index)
            else:
                landing = self.landing(self.full[k], k, (d, s - 2), index)
        i = self.ids[(k, *rest)]
        peer = self.place.neighbour(self.order[k], to)
        return self.place.copy(source, landing, self.sends.at[i], self.receives.at[i], peer)

    def arrived(self, k, s, d, index):
        if s > 1:
            return [(None, self.landing(self.full[k], k, (d, s - 2), index))]
        return [(d, self.landing(self.short[k], k, (d,), index))]

    def add(self, index, phases, more=lambda index: [], out=None):
        free = [a for a, i in zip(AXES, index, strict=True) if i is ALL]

        def one(i):
            at = {}
            for a in free[::-1]:
                at[a], i = i % self.place.dims[a], i // self.place.dims[a]
            block = [at.get(a, fixed) for a, fixed in zip(AXES, index, strict=True)]
            terms = [(None, self.own.at[tuple(block)]), (None, self.theirs.at[tuple(block)]), *more(block)]
            for k in range(phases):
                terms += [t for d in BOTH for t in self.arrived(k, self.n[k] // 2, d, block)]
            target = self.own.at[tuple(block)] if out is None else out
            for q in BOTH:
                total = None
                for columns, ref in terms:
                    if columns in (None, q):
                        value = (sub(ref, q) if columns is None else ref)[:].astype(F32)
                        total = value if total is None else total + value
                sub(target, q)[:] = total.astype(BF16)

        count = 1
        for a in free:
            count *= self.place.dims[a]
        if count == 1:
            one(0)
        else:
            pl.loop(0, count)(one)

    def send(self, k, g, s, d):
        by = (self.n[k] // 2 - s + 1) * (-1 if d else 1)
        self.add(self.index(k, g, by), k, lambda block: self.arrived(k, s - 1, d, block) if s > 1 else [])
        for w in BOTH if d is None else (d,):
            self.copy(k, g, s, w).start()

    def last(self):
        for by in range(1, self.n[2]):
            self.add(self.index(2, 0, by), 2)
            self.copy(2, by).start()

    def result(self, out):
        straight = [(None, self.straight.at[by - 1]) for by in range(1, self.n[2])]
        self.add(self.place.block, 2, lambda block: straight, out)

    def drain(self):
        for m in self.ids:
            self.copy(*m).wait_send()
        for i in range(len(self.chunks)):
            self.swap(i).wait_send()


def scatter_scratch(dims, depth, rows):
    out = []
    for order in ORDERS:
        order = order[::-1]
        *n, last = lengths(dims, order)
        out += [pltpu.VMEM((*dims, rows, depth), BF16)] * 2
        for k in BOTH:
            rest = [m for a, m in zip(AXES, dims, strict=True) if a in order[k + 1 :]]
            out.append(pltpu.VMEM((2, *rest, rows, depth // 2), BF16))
            if n[k] > 2:
                out.append(pltpu.VMEM((2, n[k] // 2 - 1, *rest, rows, depth), BF16))
        out.append(pltpu.VMEM((last - 1, rows, depth), BF16))
        out += [pltpu.SemaphoreType.DMA((len(scatter_messages(dims, order)),))] * 2
        out += [pltpu.SemaphoreType.DMA((n[0],))] * 3
    three = len(MATRICES)
    return out + [pltpu.VMEM((three, rows, depth), BF16)] * 2 + [pltpu.SemaphoreType.DMA((three,))] * 2


class UnitScatter:
    def __init__(self, place, grads, outs, scratch):
        self.place, self.outs = place, outs
        scratch = iter(scratch)
        self.matrices = [Scatter(place, m, grads[m], scratch) for m in MATRICES]
        self.mine, self.peer, self.sends, self.receives = scratch

    def prepare(self, loads):
        for m, i in loads:
            self.matrices[m].begin(i)

    def do(self, action, needs):
        what, _, m, *message = action
        matrix = self.matrices[m]
        for _, _, *need in needs:
            matrix.wait(*need)
        if what == "send":
            matrix.send(*message)
        elif what == "last":
            matrix.last()
        else:
            matrix.result(self.mine.at[m])
            self.swap(m).start()

    def swap(self, m):
        return self.place.copy(
            self.mine.at[m], self.peer.at[m], self.sends.at[m], self.receives.at[m], self.place.partner
        )

    def finish(self):
        core, other = self.place.core, self.place.other
        for m in MATRICES:
            self.swap(m).wait_recv()
            for where, ref in ((core, self.mine), (other, self.peer)):
                sums = ref[m].astype(F32)
                blocks = [sums[i : i + ROWS] for i in range(0, sums.shape[0], ROWS)]
                if m < len(MATRICES) - 1:
                    half = ROWS // 2
                    for u, block in enumerate(blocks):
                        rows = jnp.where(core == 0, block[:half], block[half:])
                        self.outs[m][where, u * half : (u + 1) * half] = rows.astype(BF16)
                else:
                    self.outs[m][where] = jnp.where(core == 0, blocks[0], blocks[-1]).astype(BF16)

    def drain(self):
        for m in MATRICES:
            self.matrices[m].drain()
            self.swap(m).wait_send()


def sums_shapes(depth, rows):
    return [jax.ShapeDtypeStruct((2, n, depth), BF16) for n in (rows // 2, rows // 2, ROWS)]


def dot(a, b, ca, cb):
    return lax.dot_general(a, b, (((ca,), (cb,)), ((), ())), preferred_element_type=F32)


def normed(h):
    wide = h.astype(F32)
    return (wide * lax.rsqrt(jnp.mean(wide * wide, -1, keepdims=True) + EPS)).astype(BF16)


def norm_backward(h, da, dh):
    wide = h.astype(F32)
    scale = lax.rsqrt(jnp.mean(wide * wide, -1, keepdims=True) + EPS)
    da = da.astype(BF16).astype(F32)
    along = jnp.mean(da * wide, -1, keepdims=True)
    dwide = scale * (da - wide * (scale * scale * along))
    return (dh.astype(F32) + dwide.astype(BF16).astype(F32)).astype(BF16)


def tile_of(matrix):
    return matrix.reshape(-1, matrix.shape[-1])


def tile_specs(dims, depth):
    nx, ny, nz = dims
    wide = pl.BlockSpec(
        (nx, ny, nz, pl.Squeezed(), ROWS, tile_width(dims)),
        lambda j: (0, 0, 0, (j % nx) * 2 // nx, j // nx, j % (nx // 2)),
    )
    tall = pl.BlockSpec((pl.Squeezed(), ny, nz, 2, ROWS, depth), lambda j: (j % nx, 0, 0, 0, j // nx, 0))
    return wide, tall


def tile_width(dims):
    return 2 * ROWS * dims[1] * dims[2]


def once(*shape):
    return pl.BlockSpec(shape, lambda j: (0,) * len(shape), pipeline_mode=pl.Buffered(1))


def backward_tile(a, dh, gate, up, down, outs, event):
    event()
    g = dot(a, gate, 1, 0)
    u = dot(a, up, 1, 0)
    s = jax.nn.sigmoid(g)
    silu = g * s
    dgate, dup, ddown = outs
    ddown[:] = dot((silu * u).astype(BF16), dh, 0, 0).astype(BF16).reshape(ddown.shape)
    dp = dot(dh, down, 1, 1).astype(BF16).astype(F32)
    du = (dp * silu).astype(BF16)
    dg = (dp * u * (s + silu * (1 - s))).astype(BF16)
    event()
    dgate[:] = dot(a, dg, 0, 0).astype(BF16).reshape(dgate.shape)
    dup[:] = dot(a, du, 0, 0).astype(BF16).reshape(dup.shape)
    return dg, du


def do_at(step, actions, work):
    if actions:

        @pl.when(pl.program_id(0) == step)
        def _():
            for action, needs in actions:
                work(action[1]).do(action, needs)


FORWARD_TIMES = (2.4, 2.1)
UNITS = ((0, 0, False), (0, 1, False), (1, 0, True))


def first_kernel(dims, plan, x, w_gate, w_up, w_down, *refs):
    refs = iter(refs)
    layer, other = [next(refs) for _ in MATRICES], [next(refs) for _ in MATRICES]
    a_out, h_out, next_out, h, a, total, p, loading, keeping, putting, putting_next = [next(refs) for _ in range(11)]
    place, units = Place(dims), []
    for l, q, flows in UNITS:
        outs = other if l else [ref.at[ALL, ALL, ALL, ALL, pl.ds(q * ROWS, ROWS)] for ref in layer]
        scratch = [next(refs) for _ in gather_scratch(dims, ROWS, flows)]
        units.append(UnitGather(place, q, flows, (w_gate.at[l, q], w_up.at[l, q], w_down.at[l]), outs, scratch))
    step, tiles = pl.program_id(0), dims[0]
    load = pltpu.make_async_copy(x, h, loading)
    keep = pltpu.make_async_copy(a, a_out, keeping)
    put_h = pltpu.make_async_copy(h, h_out, putting)
    put_next = pltpu.make_async_copy(a, next_out, putting_next)

    @pl.when(step == 0)
    def _():
        load.start()
        place.barrier()
        for unit in units:
            unit.prepare()
        load.wait()
        a[:] = normed(h[:])
        total[:] = jnp.zeros_like(total)
        keep.start()

    for u in BOTH:
        gate, up, down = units[u].buffers
        mine, steps = step // tiles == u, range(u * tiles, (u + 1) * tiles)
        for i in steps:
            do_at(i, plan[2 * i], units.__getitem__)

        @pl.when(step == u * tiles)
        def _():
            units[u].finish()

        @pl.when(mine)
        def _():
            j, width = step % tiles, tile_width(dims)
            columns = pl.ds(pl.multiple_of((j % (tiles // 2)) * width, width), width)
            core = j * 2 // tiles
            g = dot(a[:], tile_of(gate[:, :, :, core, :, columns]), 1, 0)
            p[:] = (g * jax.nn.sigmoid(g) * dot(a[:], tile_of(up[:, :, :, core, :, columns]), 1, 0)).astype(BF16)

        for i in steps:
            do_at(i, plan[2 * i + 1], units.__getitem__)

        @pl.when(mine)
        def _():
            total[:] += dot(p[:], tile_of(down[step % tiles]), 1, 0)

    do_at(2 * tiles - 1, plan[-1], units.__getitem__)

    @pl.when(step == 2 * tiles - 1)
    def _():
        keep.wait()
        out = (h[:].astype(F32) + total[:].astype(BF16).astype(F32)).astype(BF16)
        h[:] = out
        a[:] = normed(out)
        put_h.start()
        put_next.start()
        units[-1].finish()
        for unit in units:
            unit.drain()
        put_h.wait()
        put_next.wait()


def first_plan(dims, piece):
    actions, stages, begin = {}, [], {}
    for u, (*_, flows) in enumerate(UNITS):
        of_unit = gather_actions(dims, piece, u, flows)
        actions.update(of_unit)
        begin["begin", u] = 6.0
        if u in BOTH:
            stages += [(time, ()) for _ in range(dims[0]) for time in FORWARD_TIMES]
            stages[-dims[0] * len(FORWARD_TIMES)] = FORWARD_TIMES[0], of_unit
    return simulate(actions, begin, stages, gather_urgency, lead=1.5)


def first(dims, x, w_gate, w_up, w_down):
    tokens, depth = x.shape
    _, plan = first_plan(dims, 2 * ROWS * depth)
    whole = pl.BlockSpec(memory_space=pltpu.VMEM)
    outs = pl.pallas_call(
        functools.partial(first_kernel, dims, plan),
        grid=(2 * dims[0],),
        out_shape=[
            *weights_shapes(dims, depth, 2 * ROWS),
            *weights_shapes(dims, depth),
            *[jax.ShapeDtypeStruct((tokens, depth), BF16)] * 3,
        ],
        in_specs=[ANY] + [whole] * 3,
        out_specs=[ANY] * 9,
        scratch_shapes=[
            *[pltpu.VMEM((tokens, depth), kind) for kind in (BF16, BF16, F32)],
            pltpu.VMEM((tokens, tile_width(dims)), BF16),
            *[pltpu.SemaphoreType.DMA] * 4,
            *[scratch for *_, flows in UNITS for scratch in gather_scratch(dims, depth, flows)],
        ],
        compiler_params=PARAMS(collective_id=1),
        name="first",
    )(x, w_gate, w_up, w_down)
    return outs[:3], outs[3:6], outs[6:]


TILE_TIMES = (4.9, 2.5, 2.4)


def unit_kernel(dims, plan, loads, ends, a, dh, gate, up, down, *refs):
    refs = iter(refs)
    h, before = [next(refs) if end else None for end in ends]
    place, step, last = Place(dims), pl.program_id(0), pl.num_programs(0) - 1
    moved, grads = [next(refs) for _ in MATRICES], [next(refs) for _ in MATRICES]
    result = next(refs)
    arrived, total, loading = [next(refs) for _ in MATRICES], next(refs), next(refs)
    work = UnitScatter(place, moved, arrived, refs) if loads else UnitGather(place, 1, True, moved, arrived, refs)
    load = None if before is None else pltpu.make_async_copy(before, total, loading)

    @pl.when(step == 0)
    def _():
        if load is None:
            total[:] = jnp.zeros_like(total)
        else:
            load.start()
        place.barrier()
        work.prepare(loads)

    points = iter(range(len(TILE_TIMES)))

    def event():
        point = next(points)
        for i in range(dims[0]):
            do_at(i, plan[i * len(TILE_TIMES) + point], lambda unit: work)

    gate, up, down = tile_of(gate[:]), tile_of(up[:]), tile_of(down[:])
    dg, du = backward_tile(a[:], dh[:], gate, up, down, grads, event)
    event()
    if load is not None:

        @pl.when(step == 0)
        def _():
            load.wait()

    total[:] += dot(dg, gate, 1, 1) + dot(du, up, 1, 1)
    do_at(dims[0] - 1, plan[-1], lambda unit: work)

    @pl.when(step == last)
    def _():
        result[:] = total[:] if h is None else norm_backward(h[:], total[:], dh[:])
        work.finish()
        work.drain()


def unit(dims, name, a, dh, weights, moved, collective_id, h=None, before=None):
    tokens, depth = a.shape
    wide, tall = tile_specs(dims, depth)
    whole, block = once(tokens, depth), pl.BlockSpec(memory_space=pltpu.VMEM)
    piece = 2 * ROWS * depth
    stages = [(time, ()) for _ in range(dims[0]) for time in TILE_TIMES]
    if before is None:
        _, plan = simulate(gather_actions(dims, piece, 0, True), {("begin", 0): 4.0}, stages, gather_urgency)
        loads, scratch, shapes = (), gather_scratch(dims, depth, True), weights_shapes(dims, depth)
        out_specs, in_specs = ANY, block
    else:
        actions, arrivals, loads = scatter_actions(dims, piece)
        _, plan = simulate(actions, arrivals, stages, scatter_urgency)
        scratch, shapes = scatter_scratch(dims, depth, ROWS), sums_shapes(depth, ROWS)
        out_specs, in_specs = block, ANY
    ends = [(v, s) for v, s in ((h, whole), (before, ANY)) if v is not None]
    outs = pl.pallas_call(
        functools.partial(unit_kernel, dims, plan, loads, (h is not None, before is not None)),
        grid=(dims[0],),
        out_shape=[
            *weights_shapes(dims, depth),
            jax.ShapeDtypeStruct((tokens, depth), F32 if h is None else BF16),
            *shapes,
        ],
        in_specs=[whole, whole, wide, wide, tall, *[s for _, s in ends], *[in_specs] * 3],
        out_specs=[wide, wide, tall, whole, *[out_specs] * 3],
        scratch_shapes=[pltpu.VMEM((tokens, depth), F32), pltpu.SemaphoreType.DMA, *scratch],
        compiler_params=PARAMS(collective_id=collective_id),
        name=name,
    )(a, dh, *weights, *[v for v, _ in ends], *moved)
    return outs[:3], outs[3], outs[4:]


def layer_kernel(dims, plan, loads, a, dh, gate, up, down, *refs):
    refs = iter(refs)
    moved, grads = [next(refs) for _ in MATRICES], [next(refs) for _ in MATRICES]
    dg_out, du_out = next(refs), next(refs)
    arrived, place, step = [next(refs) for _ in MATRICES], Place(dims), pl.program_id(0)
    work = UnitScatter(place, moved, arrived, refs)

    @pl.when(step == 0)
    def _():
        place.barrier()
        work.prepare(loads)

    points = iter(BOTH)

    def event():
        point = next(points)
        for i in range(2 * dims[0]):
            do_at(i, plan[2 * i + point], lambda unit: work)

    dg_out[:], du_out[:] = backward_tile(
        a[:], dh[:], tile_of(gate[:]), tile_of(up[:]), tile_of(down[:]), grads, event
    )
    do_at(2 * dims[0] - 1, plan[-1], lambda unit: work)

    @pl.when(step == 2 * dims[0] - 1)
    def _():
        work.finish()
        work.drain()


def layer(dims, a, dh, weights, moved, collective_id):
    tokens, depth = a.shape
    wide, tall = tile_specs(dims, depth)
    width = tile_width(dims)
    whole, block = once(tokens, depth), pl.BlockSpec(memory_space=pltpu.VMEM)
    part = pl.BlockSpec((tokens, width), lambda j: (0, j))
    actions, arrivals, loads = scatter_actions(dims, 2 * ROWS * depth)
    stages = [(time, ()) for _ in range(2 * dims[0]) for time in TILE_TIMES[:2]]
    _, plan = simulate(actions, arrivals, stages, scatter_urgency)
    outs = pl.pallas_call(
        functools.partial(layer_kernel, dims, plan, loads),
        grid=(2 * dims[0],),
        out_shape=[
            *weights_shapes(dims, depth, 2 * ROWS),
            *[jax.ShapeDtypeStruct((tokens, 2 * dims[0] * width), BF16)] * 2,
            *sums_shapes(depth, ROWS),
        ],
        in_specs=[whole, whole, wide, wide, tall] + [ANY] * 3,
        out_specs=[wide, wide, tall, part, part] + [block] * 3,
        scratch_shapes=scatter_scratch(dims, depth, ROWS),
        compiler_params=PARAMS(collective_id=collective_id),
        name="layer",
    )(a, dh, *weights, *moved)
    return outs[:3], outs[3:5], outs[5:]


def last_kernel(dims, plan, loads, h, dh, dg, du, gate, up, *refs):
    refs = iter(refs)
    moved, dx = [next(refs) for _ in MATRICES], next(refs)
    arrived, total, loading = [next(refs) for _ in MATRICES], next(refs), next(refs)
    place, step, tiles = Place(dims), pl.program_id(0), 2 * dims[0]
    work = UnitScatter(place, moved, arrived, refs)
    load = pltpu.make_async_copy(h, dx, loading)

    @pl.when(step == 0)
    def _():
        load.start()
        place.barrier()
        work.prepare(loads)
        total[:] = jnp.zeros_like(total)

    for i in range(tiles):
        do_at(i, plan[i], lambda unit: work)
    total[:] += dot(dg[:], tile_of(gate[:]), 1, 1) + dot(du[:], tile_of(up[:]), 1, 1)

    @pl.when(step == tiles - 1)
    def _():
        load.wait()
        dx[:] = norm_backward(dx[:], total[:], dh[:])

    do_at(tiles - 1, plan[-1], lambda unit: work)

    @pl.when(step == tiles - 1)
    def _():
        work.finish()
        work.drain()


def last(dims, h, dh, for_projections, weights, moved, collective_id):
    tokens, depth = h.shape
    wide, _ = tile_specs(dims, depth)
    whole, block = once(tokens, depth), pl.BlockSpec(memory_space=pltpu.VMEM)
    part = pl.BlockSpec((tokens, tile_width(dims)), lambda j: (0, j))
    actions, arrivals, loads = scatter_actions(dims, 4 * ROWS * depth)
    tiles = 2 * dims[0]
    _, plan = simulate(actions, arrivals, [(TILE_TIMES[-1], ())] * tiles, scatter_urgency)
    dx, *sums = pl.pallas_call(
        functools.partial(last_kernel, dims, plan, loads),
        grid=(tiles,),
        out_shape=[jax.ShapeDtypeStruct((tokens, depth), BF16), *sums_shapes(depth, 2 * ROWS)],
        in_specs=[ANY, whole, part, part, wide, wide] + [ANY] * 3,
        out_specs=[whole] + [block] * 3,
        scratch_shapes=[
            pltpu.VMEM((tokens, depth), F32),
            pltpu.SemaphoreType.DMA,
            *scatter_scratch(dims, depth, 2 * ROWS),
        ],
        compiler_params=PARAMS(collective_id=collective_id),
        name="last",
    )(h, dh, *for_projections, *weights[:2], *moved)
    return dx, sums


def solution(mesh):
    dims = DIMS[mesh.shape["dp"]]
    half_chips = dims[0] * dims[1] * dims[2] // 2

    def split(w):
        layers, rows, _ = w.shape
        w = w.reshape(layers, rows, 2, half_chips, 2, 2 * ROWS)
        return w.transpose(0, 4, 2, 1, 3, 5).reshape(layers, 2, 2, rows, -1)

    def join(first, halves):
        w = jnp.stack([first, jnp.concatenate(halves, 1)])
        w = w.reshape(2, 2, 2, ROWS // 2, half_chips, 2 * ROWS)
        return w.transpose(0, 3, 1, 4, 2, 5).reshape(2, ROWS // 2, -1)

    def local(x, dy, w_gate, w_up, w_down):
        h, dh = x[0], dy[0]
        shards = split(w_gate), split(w_up), w_down.reshape(2, 2, ROWS, -1)
        weights1, weights2a, (a1, h1, a2) = first(dims, h, *shards)
        moved = shards[0][1, 1], shards[1][1, 1], shards[2][1]
        terms, before, weights2b = unit(dims, "second", a2, dh, weights2a, moved, 2)
        terms, dh1, (gate2a, up2a, down2a) = unit(dims, "third", a2, dh, weights2b, terms, 3, h=h1, before=before)
        terms, for_projections, (gate2b, up2b, down2b) = layer(dims, a1, dh1, weights1, terms, 4)
        dh0, (gate1, up1, down1) = last(dims, h, dh1, for_projections, weights1, terms, 5)
        down2 = jnp.where(lax.axis_index("dp") % 2 == 0, down2a, down2b)
        down = jnp.stack([down1, down2]).reshape(2, 2 * ROWS, -1)
        return dh0[None], join(gate1, (gate2a, gate2b)), join(up1, (up2a, up2b)), down

    rows, sequences = P(None, "dp"), P(("rep", "dp"))
    return jax.shard_map(
        local,
        mesh=mesh,
        in_specs=(sequences,) * 2 + (rows,) * 3,
        out_specs=(sequences,) + (P("rep", "dp"),) * 3,
        check_vma=False,
    )
```
